512 devices in a mesh: rep: 16 (over y, x_hi, core), fsdp: 32 (over x_lo, z).
Axes of the slice: x: 4 (x_hi: 2, x_lo: 2; x = x_hi * 2 + x_lo), y: 4, z: 16, core: 2. Of those that a mesh axis runs over, the one named last changes fastest.
Arguments:
- activations: bfloat16 [16, 4096, 64], P('rep', 'fsdp'), may hold values from -6 to 6
- out_grads: bfloat16 [16, 4096, 14848], P('rep', 'fsdp'), may hold values from -0.25 to 0.25
- params: float32 [16, 64, 14848], P('rep', 'fsdp'), may hold values from -6 to 6
- first_moment: float32 [16, 64, 14848], P('rep', 'fsdp'), may hold values from -6 to 6
- second_moment: float32 [16, 64, 14848], P('rep', 'fsdp'), may hold values from 0.5 to 8
Outputs:
- mean_params: float32 [64, 14848], P('fsdp')
- mean_first: float32 [64, 14848], P('fsdp')
- mean_second: float32 [64, 14848], P('fsdp')
The draws below stay inside these ranges and needn't reach their ends.
All inputs are finite; a program needn't handle non-finite values.
Results may differ from the reference program's by a relative error of at most 0.0003.
Values may be sent and summed in bfloat16 or wider, within the bound.
No kernel may reach another device: no remote copies, remote signals or barrier semaphores. Data moves between devices by JAX's collectives and lax.ppermute only.
A program may use at most 64 MiB of HBM per device.

```python
import math
import jax
import jax.numpy as jnp
from jax import lax

HID = 14848
STEP = 100
D = 64
TOKENS = 4096
REPS = 16


def level_of(own_key, dims, pieces, smallest, top_value):
    factor_of, own = 1.0, jax.random.fold_in(own_key, 6)
    for position, parts in pieces:
        draws = jnp.exp(jax.random.uniform(jax.random.fold_in(own, position), (parts,), jnp.float32, smallest / len(pieces), top_value / len(pieces)))
        factor_of = factor_of * jnp.repeat(draws, dims[position] // parts).reshape([-1 if axis == position else 1 for axis in range(len(dims))])
    return factor_of


def noise(key, shape, scale, bound, cuts=(), dtype=jnp.bfloat16):
    drawn = scale * jax.random.normal(key, shape, jnp.float32)
    if cuts:
        drawn = drawn * level_of(key, shape, cuts, -0.22, 0.18)
    return jnp.clip(drawn, -bound, bound).astype(dtype)


def setup_inputs(seed: int = 0) -> dict:
    keys = jax.random.split(jax.random.key(seed), 6)
    return {
        "activations": noise(keys[0], (REPS, TOKENS, D), 1.0, 6.0, ((0, 16), (1, 32))),
        "out_grads": noise(keys[1], (REPS, TOKENS, HID), (TOKENS // 9) ** -0.5, 0.25, ((0, 16), (1, 32))),
        "params": noise(keys[2], (REPS, D, HID), 1.0, 6.0, ((0, 16), (1, 32)), jnp.float32),
        "first_moment": noise(keys[3], (REPS, D, HID), 1.0, 6.0, ((0, 16), (1, 32)), jnp.float32),
        "second_moment": jnp.clip(jnp.exp(math.log(8.0) - 2.7725887 * jax.random.uniform(keys[4], (REPS, D, HID), jnp.float32) ** level_of(keys[4], (REPS, D, HID), ((0, 16), (1, 32)), -0.2, 0.2)), 0.5, 8.0),
    }


def one_replica(x, dy, p, m, v):
    grad = lax.dot_general(x, dy, (((0,), (0,)), ((), ())), preferred_element_type=jnp.float32)
    new_first = 0.9 * m + 0.1 * grad
    new_second = 0.95 * v + 0.05 * grad * grad
    corr_first = 1.0 - 0.9 ** STEP
    corr_second = 1.0 - 0.95 ** STEP
    update = new_first / corr_first / (jnp.sqrt(new_second / corr_second) + 1e-08)
    new_params = p - 0.01 * (update + 0.1 * p)
    return (new_params, new_first, new_second)

def reference(activations, out_grads, params, first_moment, second_moment):
    total_p = jnp.zeros((D, HID), jnp.float32)
    total_m = jnp.zeros((D, HID), jnp.float32)
    total_v = jnp.zeros((D, HID), jnp.float32)
    for replica in range(REPS):
        p1, m1, v1 = one_replica(activations[replica], out_grads[replica], params[replica], first_moment[replica], second_moment[replica])
        total_p = total_p + p1
        total_m = total_m + m1
        total_v = total_v + v1
    return (total_p / REPS, total_m / REPS, total_v / REPS)
```

```python
import jax
import jax.numpy as jnp
from jax import lax
from jax.sharding import Mesh
from jax.sharding import PartitionSpec as P

STEP = 100
FSDP = ("x", "z")
CHUNKS = 2


def contract_tokens(left, right):
    return lax.dot_general(
        left, right, (((0,), (0,)), ((), ())), preferred_element_type=jnp.float32
    )


def spread(feats, blocks):
    tokens, width = feats.shape
    rows = width // (2 * blocks)
    own = feats.reshape(tokens, 2, blocks, rows).transpose(0, 2, 1, 3)[..., None]
    none = jnp.zeros_like(own)
    first = jnp.concatenate([own, none], axis=-1).reshape(tokens, -1)
    second = jnp.concatenate([none, own], axis=-1).reshape(tokens, -1)
    return first, second


def ring_sums(parts, axis):
    count = lax.axis_size(axis)
    here = lax.axis_index(axis)
    up = [(i, (i + 1) % count) for i in range(count)]
    down = [(i, (i - 1) % count) for i in range(count)]

    def block(part, k):
        return lax.dynamic_index_in_dim(part, lax.rem(k + 2 * count, count), 0, False)

    lanes = []
    for c, part in enumerate(parts):
        far = count // 2
        hops = (far, count - 1 - far) if c % 2 == 0 else (count - 1 - far, far)
        lanes.append([c, 1, up, hops[0], block(part, here + hops[0])])
        lanes.append([c, -1, down, hops[1], block(part, here - hops[1])])
    for s in range(count // 2):
        for lane in lanes:
            c, sign, perm, hops, acc = lane
            if s < hops:
                got = lax.ppermute(acc, axis, perm)
                left = hops - s - 1
                lane[4] = got + block(parts[c], here + sign * left) if left else got
    return [
        lanes[2 * c][4] + lanes[2 * c + 1][4] + block(part, here)
        for c, part in enumerate(parts)
    ]


def pair_sum(array, axis):
    half = array.shape[0] // 2
    low, high = array[:half], array[half:]
    first = lax.axis_index(axis) == 0
    mine, other = jnp.where(first, low, high), jnp.where(first, high, low)
    return mine + lax.ppermute(other, axis, [(0, 1), (1, 0)])


def mean_over(arrays, axis):
    count = lax.axis_size(axis)
    flat = jnp.concatenate([a.reshape(-1) for a in arrays])
    tiles = flat.reshape(count, -1)
    arrived = lax.all_to_all(tiles, axis, 0, 0, tiled=True).sum(axis=0) / count
    whole = lax.all_to_all(
        jnp.broadcast_to(arrived[None], tiles.shape), axis, 0, 0, tiled=True
    ).reshape(-1)
    size = arrays[0].size
    return [whole[i * size : (i + 1) * size].reshape(a.shape) for i, a in enumerate(arrays)]


def per_device(activations, out_grads, params, first_moment, second_moment):
    blocks = lax.axis_size("z")
    feats, grads_out = activations[0], out_grads[0]
    shape = params.shape[1:]
    half = shape[1] // 2
    width = half // CHUNKS
    left = spread(feats, blocks)
    parts = []
    for c in range(CHUNKS):
        total = sum(
            contract_tokens(left[h], lax.slice_in_dim(grads_out, at, at + width, axis=1))
            for h, at in ((0, c * width), (1, half + c * width))
        )
        parts.append(total.reshape(blocks, -1, width))
    grad = jnp.concatenate([pair_sum(a, "x") for a in ring_sums(parts, "z")], axis=1)

    def fold(a):
        return a[0].reshape(grad.shape)

    weights, moment_one, moment_two = fold(params), fold(first_moment), fold(second_moment)
    new_first = 0.9 * moment_one + 0.1 * grad
    new_second = 0.95 * moment_two + 0.05 * grad * grad
    corr_first = 1.0 - 0.9**STEP
    corr_second = 1.0 - 0.95**STEP
    update = new_first / corr_first / (jnp.sqrt(new_second / corr_second) + 1e-08)
    new_params = weights - 0.01 * (update + 0.1 * weights)
    means = mean_over((new_params, new_first, new_second), "rep")
    return tuple(a.reshape(shape) for a in means)


def solution(mesh):
    split = Mesh(mesh.devices.reshape(mesh.shape["rep"], 2, 16), ("rep", "x", "z"))
    spec = P("rep", FSDP, None)
    out = P(FSDP, None)
    return jax.shard_map(
        per_device,
        mesh=split,
        in_specs=(spec,) * 5,
        out_specs=(out,) * 3,
        check_vma=False,
    )
```

```python
import jax
import jax.numpy as jnp
from jax import lax
from jax.sharding import Mesh
from jax.sharding import PartitionSpec as P

STEP = 100
FSDP = ("x", "z")
CHUNKS = 2


def contract_tokens(left, right):
    return lax.dot_general(
        left, right, (((0,), (0,)), ((), ())), preferred_element_type=jnp.float32
    )


def spread(feats, blocks):
    tokens, width = feats.shape
    rows = width // (2 * blocks)
    own = feats.reshape(tokens, 2, blocks, rows).transpose(0, 2, 1, 3)[..., None]
    none = jnp.zeros_like(own)
    first = jnp.concatenate([own, none], axis=-1).reshape(tokens, -1)
    second = jnp.concatenate([none, own], axis=-1).reshape(tokens, -1)
    return first, second


def ring_sums(parts, axis):
    count = lax.axis_size(axis)
    far = count // 2
    here = lax.axis_index(axis)
    side = 1 - 2 * lax.rem(here, 2)
    swaps = [
        [(i, (i + step) % count) for i in range(count) for step in (1 if (i + k) % 2 == 0 else -1,)]
        for k in range(2)
    ]

    def block(c, distance):
        k = here + (side if c % 2 == 0 else -side) * distance
        return lax.dynamic_index_in_dim(parts[c], k & (count - 1), 0, False)

    def swap(array, c, which):
        return lax.ppermute(array, axis, swaps[(c + which) % 2])

    chunks = range(len(parts))
    arrived = [(None, swap(block(c, far), c, 0)) for c in chunks]
    for left in range(far - 1, 0, -1):
        for c in chunks:
            from_second, from_first = arrived[c]
            ahead, behind = block(c, left), from_first + block(c, -left)
            if from_second is not None:
                ahead = from_second + ahead
            first = swap(ahead, c, 0)
            arrived[c] = (swap(behind, c, 1), first)
    return [arrived[c][0] + arrived[c][1] + block(c, 0) for c in chunks]


def pair_sum(array, axis):
    half = array.shape[0] // 2
    low, high = array[:half], array[half:]
    first = lax.axis_index(axis) == 0
    mine, other = jnp.where(first, low, high), jnp.where(first, high, low)
    return mine + lax.ppermute(other, axis, [(0, 1), (1, 0)])


def mean_over(arrays, axis):
    count = lax.axis_size(axis)
    flat = jnp.concatenate([a.reshape(-1) for a in arrays])
    tiles = flat.reshape(count, -1)
    arrived = lax.all_to_all(tiles, axis, 0, 0, tiled=True).sum(axis=0) / count
    whole = lax.all_to_all(
        jnp.broadcast_to(arrived[None], tiles.shape), axis, 0, 0, tiled=True
    ).reshape(-1)
    size = arrays[0].size
    return [whole[i * size : (i + 1) * size].reshape(a.shape) for i, a in enumerate(arrays)]


def per_device(activations, out_grads, params, first_moment, second_moment):
    blocks = lax.axis_size("z")
    feats, grads_out = activations[0], out_grads[0]
    shape = params.shape[1:]
    half = shape[1] // 2
    width = half // CHUNKS
    left = spread(feats, blocks)
    parts = []
    for c in range(CHUNKS):
        total = sum(
            contract_tokens(left[h], lax.slice_in_dim(grads_out, at, at + width, axis=1))
            for h, at in ((0, c * width), (1, half + c * width))
        )
        parts.append(total.reshape(blocks, -1, width))
    grad = jnp.concatenate([pair_sum(a, "x") for a in ring_sums(parts, "z")], axis=1)

    def fold(a):
        return a[0].reshape(grad.shape)

    weights, moment_one, moment_two = fold(params), fold(first_moment), fold(second_moment)
    new_first = 0.9 * moment_one + 0.1 * grad
    new_second = 0.95 * moment_two + 0.05 * grad * grad
    corr_first = 1.0 - 0.9**STEP
    corr_second = 1.0 - 0.95**STEP
    update = new_first / corr_first / (jnp.sqrt(new_second / corr_second) + 1e-08)
    new_params = weights - 0.01 * (update + 0.1 * weights)
    means = mean_over((new_params, new_first, new_second), "rep")
    return tuple(a.reshape(shape) for a in means)


def solution(mesh):
    split = Mesh(mesh.devices.reshape(mesh.shape["rep"], 2, 16), ("rep", "x", "z"))
    spec = P("rep", FSDP, None)
    out = P(FSDP, None)
    return jax.shard_map(
        per_device,
        mesh=split,
        in_specs=(spec,) * 5,
        out_specs=(out,) * 3,
        check_vma=False,
    )
```

```python
import jax
import jax.numpy as jnp
from jax import lax
from jax.sharding import Mesh
from jax.sharding import PartitionSpec as P

STEP = 100
FSDP = ("x", "z")


def contract_tokens(left, right):
    return lax.dot_general(
        left, right, (((0,), (0,)), ((), ())), preferred_element_type=jnp.float32
    )


def spread(feats, blocks, place):
    tokens, width = feats.shape
    rows = width // (2 * blocks)
    shape = (width, 4 * width)
    source, column = (lax.broadcasted_iota(jnp.int32, shape, i) for i in range(2))
    group = column // (2 * width)
    block = (column // (4 * rows)) % blocks
    pair = (column // (2 * rows)) % 2
    row = (column // 2) % rows
    wanted = (pair * blocks + place(block)) * rows + row
    chosen = (source == wanted) & (group == column % 2)
    picked = jnp.dot(feats, chosen.astype(feats.dtype), preferred_element_type=jnp.float32)
    return picked.astype(feats.dtype).reshape(tokens, 2, blocks, -1)


def block_sums(left, grads_out):
    half = grads_out.shape[1] // 2
    total = sum(
        contract_tokens(
            left[:, h].reshape(left.shape[0], -1),
            lax.slice_in_dim(grads_out, h * half, (h + 1) * half, axis=1),
        )
        for h in range(2)
    )
    return total.reshape(left.shape[2], -1, half)


def ring_sum(left, grads_out, axis):
    count = lax.axis_size(axis)
    far = count // 2
    swaps = [
        [(i, (i + step) % count) for i in range(count) for step in (1 if (i + k) % 2 == 0 else -1,)]
        for k in range(2)
    ]
    start = block_sums(left[:, :, :1], grads_out)[0]
    from_first = lax.ppermute(start, axis, swaps[0])
    long = block_sums(left[:, :, 1:far], grads_out)
    short = block_sums(left[:, :, far:], grads_out)
    for s in range(1, far):
        if s == 1:
            one, two = lax.optimization_barrier((from_first + long[0], short[0]))
        else:
            one, two = one + long[s - 1], two + short[s - 1]
        one = lax.ppermute(one, axis, swaps[s % 2])
        two = lax.ppermute(two, axis, swaps[(s + 1) % 2])
    return one + two + short[far - 1]


def pair_sum(array, axis):
    half = array.shape[0] // 2
    low, high = array[:half], array[half:]
    first = lax.axis_index(axis) == 0
    mine, other = jnp.where(first, low, high), jnp.where(first, high, low)
    return mine + lax.ppermute(other, axis, [(0, 1), (1, 0)])


def mean_over(arrays, axis):
    count = lax.axis_size(axis)
    flat = jnp.concatenate([a.reshape(-1) for a in arrays])
    tiles = flat.reshape(count, -1)
    arrived = lax.all_to_all(tiles, axis, 0, 0, tiled=True).sum(axis=0) / count
    whole = lax.all_to_all(
        jnp.broadcast_to(arrived[None], tiles.shape), axis, 0, 0, tiled=True
    ).reshape(-1)
    size = arrays[0].size
    return [whole[i * size : (i + 1) * size].reshape(a.shape) for i, a in enumerate(arrays)]


def per_device(activations, out_grads, params, first_moment, second_moment):
    blocks = lax.axis_size("z")
    feats, grads_out = activations[0], out_grads[0]
    shape = params.shape[1:]
    here = lax.axis_index("z")
    side = 1 - 2 * lax.rem(here, 2)
    far = blocks // 2

    def place(i):
        late = i // far
        sign = 2 * (i & 1) - 1
        return (here + side * (far + sign * (i % far + late))) & (blocks - 1)

    left = spread(feats, blocks, place)
    grad = pair_sum(ring_sum(left, grads_out, "z"), "x")

    def fold(a):
        return a[0].reshape(grad.shape)

    weights, moment_one, moment_two = fold(params), fold(first_moment), fold(second_moment)
    new_first = 0.9 * moment_one + 0.1 * grad
    new_second = 0.95 * moment_two + 0.05 * grad * grad
    corr_first = 1.0 - 0.9**STEP
    corr_second = 1.0 - 0.95**STEP
    update = new_first / corr_first / (jnp.sqrt(new_second / corr_second) + 1e-08)
    new_params = weights - 0.01 * (update + 0.1 * weights)
    means = mean_over((new_params, new_first, new_second), "rep")
    return tuple(a.reshape(shape) for a in means)


def solution(mesh):
    split = Mesh(mesh.devices.reshape(mesh.shape["rep"], 2, 16), ("rep", "x", "z"))
    spec = P("rep", FSDP, None)
    out = P(FSDP, None)
    return jax.shard_map(
        per_device,
        mesh=split,
        in_specs=(spec,) * 5,
        out_specs=(out,) * 3,
        check_vma=False,
    )
```

```python
import jax
import jax.numpy as jnp
from jax import lax
from jax.sharding import Mesh
from jax.sharding import PartitionSpec as P

STEP = 100
FSDP = ("x", "z")


def contract_tokens(left, right):
    return lax.dot_general(
        left, right, (((0,), (0,)), ((), ())), preferred_element_type=jnp.float32
    )


def spread(feats, blocks, place):
    tokens, width = feats.shape
    rows = width // (2 * blocks)
    shape = (width, 4 * width)
    source, column = (lax.broadcasted_iota(jnp.int32, shape, i) for i in range(2))
    group = column // (2 * width)
    block = (column // (4 * rows)) % blocks
    pair = (column // (2 * rows)) % 2
    row = (column // 2) % rows
    wanted = (pair * blocks + place(block)) * rows + row
    chosen = (source == wanted) & (group == column % 2)
    picked = jnp.dot(feats, chosen.astype(feats.dtype), preferred_element_type=jnp.float32)
    return picked.astype(feats.dtype).reshape(tokens, 2, blocks, -1)


def block_sums(left, grads_out):
    half = grads_out.shape[1] // 2
    total = sum(
        contract_tokens(
            left[:, h].reshape(left.shape[0], -1),
            lax.slice_in_dim(grads_out, h * half, (h + 1) * half, axis=1),
        )
        for h in range(2)
    )
    return total.reshape(left.shape[2], -1, half)


def keep_and_give(array, axis):
    half = array.shape[0] // 2
    low, high = array[:half], array[half:]
    first = lax.axis_index(axis) == 0
    return jnp.where(first, low, high), jnp.where(first, high, low)


def owned_sum(left, grads_out, axis, pair):
    count = lax.axis_size(axis)
    far = count // 2
    swaps = [
        [(i, (i + step) % count) for i in range(count) for step in (1 if (i + k) % 2 == 0 else -1,)]
        for k in range(2)
    ]
    across = [(0, 1), (1, 0)]
    start = block_sums(left[:, :, :1], grads_out)[0]
    start, left = lax.optimization_barrier((start, left))
    one = lax.ppermute(start, axis, swaps[0])
    short = block_sums(left[:, :, far:], grads_out)
    long = block_sums(left[:, :, 1:far], grads_out)
    two, long = lax.optimization_barrier((short[0], long))
    for s in range(1, far):
        one = one + long[s - 1]
        if s < far - 1:
            one = lax.ppermute(one, axis, swaps[s % 2])
        two = lax.ppermute(two, axis, swaps[(s + 1) % 2]) + short[s]
    kept, given = keep_and_give(one, pair)
    last = swaps[(far - 1) % 2]
    slant = [(p * count + i, q * count + j) for p, q in across for i, j in last]
    aside = lax.ppermute(given, (pair, axis), slant)
    along = lax.ppermute(kept, axis, last)
    kept, given = keep_and_give(two, pair)
    return along + aside + (kept + lax.ppermute(given, pair, across))


def mean_over(arrays, axis):
    count = lax.axis_size(axis)
    flat = jnp.concatenate([a.reshape(-1) for a in arrays])
    tiles = flat.reshape(count, -1)
    arrived = lax.all_to_all(tiles, axis, 0, 0, tiled=True).sum(axis=0) / count
    whole = lax.all_to_all(
        jnp.broadcast_to(arrived[None], tiles.shape), axis, 0, 0, tiled=True
    ).reshape(-1)
    size = arrays[0].size
    return [whole[i * size : (i + 1) * size].reshape(a.shape) for i, a in enumerate(arrays)]


def per_device(activations, out_grads, params, first_moment, second_moment):
    blocks = lax.axis_size("z")
    feats, grads_out = activations[0], out_grads[0]
    shape = params.shape[1:]
    here = lax.axis_index("z")
    side = 1 - 2 * lax.rem(here, 2)
    far = blocks // 2

    def place(i):
        late = i // far
        sign = 2 * (i & 1) - 1
        return (here + side * (far + sign * (i % far + late))) & (blocks - 1)

    left = spread(feats, blocks, place)
    grad = owned_sum(left, grads_out, "z", "x")

    def fold(a):
        return a[0].reshape(grad.shape)

    weights, moment_one, moment_two = fold(params), fold(first_moment), fold(second_moment)
    new_first = 0.9 * moment_one + 0.1 * grad
    new_second = 0.95 * moment_two + 0.05 * grad * grad
    corr_first = 1.0 - 0.9**STEP
    corr_second = 1.0 - 0.95**STEP
    update = new_first / corr_first / (jnp.sqrt(new_second / corr_second) + 1e-08)
    new_params = weights - 0.01 * (update + 0.1 * weights)
    means = mean_over((new_params, new_first, new_second), "rep")
    return tuple(a.reshape(shape) for a in means)


def solution(mesh):
    split = Mesh(mesh.devices.reshape(mesh.shape["rep"], 2, 16), ("rep", "x", "z"))
    spec = P("rep", FSDP, None)
    out = P(FSDP, None)
    return jax.shard_map(
        per_device,
        mesh=split,
        in_specs=(spec,) * 5,
        out_specs=(out,) * 3,
        check_vma=False,
    )
```

```python
import jax
import jax.numpy as jnp
from jax import lax
from jax.sharding import Mesh
from jax.sharding import PartitionSpec as P

STEP = 100
FSDP = ("x", "z")


def contract_tokens(left, right):
    return lax.dot_general(
        left, right, (((0,), (0,)), ((), ())), preferred_element_type=jnp.float32
    )


def spread(feats, blocks, place):
    tokens, width = feats.shape
    rows = width // (2 * blocks)
    shape = (width, 4 * width)
    source, column = (lax.broadcasted_iota(jnp.int32, shape, i) for i in range(2))
    group = column // (2 * width)
    block = (column // (4 * rows)) % blocks
    pair = (column // (2 * rows)) % 2
    row = (column // 2) % rows
    wanted = (pair * blocks + place(block)) * rows + row
    chosen = (source == wanted) & (group == column % 2)
    picked = jnp.dot(feats, chosen.astype(feats.dtype), preferred_element_type=jnp.float32)
    return picked.astype(feats.dtype).reshape(tokens, 2, blocks, -1)


def block_sums(left, grads_out):
    half = grads_out.shape[1] // 2
    total = sum(
        contract_tokens(
            left[:, h].reshape(left.shape[0], -1),
            lax.slice_in_dim(grads_out, h * half, (h + 1) * half, axis=1),
        )
        for h in range(2)
    )
    return total.reshape(left.shape[2], -1, half)


def keep_and_give(array, axis):
    half = array.shape[0] // 2
    low, high = array[:half], array[half:]
    first = lax.axis_index(axis) == 0
    return jnp.where(first, low, high), jnp.where(first, high, low)


def owned_sum(left, grads_out, axis, pair):
    count = lax.axis_size(axis)
    far = count // 2
    swaps = [
        [(i, (i + step) % count) for i in range(count) for step in (1 if (i + k) % 2 == 0 else -1,)]
        for k in range(2)
    ]
    across = [(0, 1), (1, 0)]

    def to_owners(array, which):
        kept, given = keep_and_give(array, pair)
        slant = [(p * count + i, q * count + j) for p, q in across for i, j in swaps[which]]
        aside = lax.ppermute(given, (pair, axis), slant)
        return lax.ppermute(kept, axis, swaps[which]) + aside

    start = block_sums(left[:, :, :1], grads_out)[0]
    start, left = lax.optimization_barrier((start, left))
    one = lax.ppermute(start, axis, swaps[0])
    short = block_sums(left[:, :, far:], grads_out)
    long = block_sums(left[:, :, 1:far], grads_out)
    two, long = lax.optimization_barrier((short[0], long))
    for s in range(1, far - 1):
        one = lax.ppermute(one + long[s - 1], axis, swaps[s % 2])
        two = lax.ppermute(two, axis, swaps[(s + 1) % 2]) + short[s]
        if s == 2:
            kept, given = keep_and_give(short[far - 1], pair)
            given, two = lax.optimization_barrier((given, two))
            own = kept + lax.ppermute(given, pair, across)
    two = own + to_owners(two, far % 2)
    return to_owners(one + long[far - 2], (far - 1) % 2) + two


def mean_over(arrays, axis):
    count = lax.axis_size(axis)
    flat = jnp.concatenate([a.reshape(-1) for a in arrays])
    tiles = flat.reshape(count, -1)
    arrived = lax.all_to_all(tiles, axis, 0, 0, tiled=True).sum(axis=0) / count
    whole = lax.all_to_all(
        jnp.broadcast_to(arrived[None], tiles.shape), axis, 0, 0, tiled=True
    ).reshape(-1)
    size = arrays[0].size
    return [whole[i * size : (i + 1) * size].reshape(a.shape) for i, a in enumerate(arrays)]


def per_device(activations, out_grads, params, first_moment, second_moment):
    blocks = lax.axis_size("z")
    feats, grads_out = activations[0], out_grads[0]
    shape = params.shape[1:]
    here = lax.axis_index("z")
    side = 1 - 2 * lax.rem(here, 2)
    far = blocks // 2

    def place(i):
        late = i // far
        sign = 2 * (i & 1) - 1
        return (here + side * (far + sign * (i % far + late))) & (blocks - 1)

    left = spread(feats, blocks, place)
    grad = owned_sum(left, grads_out, "z", "x")

    def fold(a):
        return a[0].reshape(grad.shape)

    weights, moment_one, moment_two = fold(params), fold(first_moment), fold(second_moment)
    new_first = 0.9 * moment_one + 0.1 * grad
    new_second = 0.95 * moment_two + 0.05 * grad * grad
    corr_first = 1.0 - 0.9**STEP
    corr_second = 1.0 - 0.95**STEP
    update = new_first / corr_first / (jnp.sqrt(new_second / corr_second) + 1e-08)
    new_params = weights - 0.01 * (update + 0.1 * weights)
    means = mean_over((new_params, new_first, new_second), "rep")
    return tuple(a.reshape(shape) for a in means)


def solution(mesh):
    split = Mesh(mesh.devices.reshape(mesh.shape["rep"], 2, 16), ("rep", "x", "z"))
    spec = P("rep", FSDP, None)
    out = P(FSDP, None)
    return jax.shard_map(
        per_device,
        mesh=split,
        in_specs=(spec,) * 5,
        out_specs=(out,) * 3,
        check_vma=False,
    )
```

```python
import jax
import jax.numpy as jnp
from jax import lax
from jax.experimental import pallas as pl
from jax.experimental.pallas import tpu as pltpu
from jax.sharding import Mesh
from jax.sharding import PartitionSpec as P

STEP = 100
FSDP = ("x", "z")


def spread(feats, blocks, place):
    tokens, width = feats.shape
    rows = width // (2 * blocks)
    shape = (width, 4 * width)
    source, column = (lax.broadcasted_iota(jnp.int32, shape, i) for i in range(2))
    group = column // (2 * width)
    block = (column // (4 * rows)) % blocks
    pair = (column // (2 * rows)) % 2
    row = (column // 2) % rows
    wanted = (pair * blocks + place(block)) * rows + row
    chosen = (source == wanted) & (group == column % 2)
    picked = lax.dot_general(
        chosen.astype(feats.dtype),
        feats,
        (((0,), (1,)), ((), ())),
        preferred_element_type=jnp.float32,
    )
    return picked.astype(feats.dtype)


STRIP = 512


def block_sums(left, grads_out, sizes):
    tokens, hidden = grads_out.shape
    half = hidden // 2
    rows = sum(sizes)

    def kernel(left_ref, grads_ref, *out_refs):
        for at in range(0, half, STRIP):
            size = min(STRIP, half - at)
            total = sum(
                jnp.dot(
                    left_ref[pl.ds(h * rows, rows), :],
                    grads_ref[:, pl.ds(h * half + at, size)],
                    preferred_element_type=jnp.float32,
                )
                for h in range(2)
            )
            first = 0
            for ref, count in zip(out_refs, sizes):
                ref[:, pl.ds(at, size)] = total[first : first + count]
                first += count

    vmem = pl.BlockSpec(memory_space=pltpu.VMEM)
    return pl.pallas_call(
        kernel,
        in_specs=[vmem, vmem],
        out_specs=[vmem] * len(sizes),
        out_shape=[jax.ShapeDtypeStruct((n, half), jnp.float32) for n in sizes],
        compiler_params=pltpu.CompilerParams(vmem_limit_bytes=24 * 2**20),
        cost_estimate=pl.CostEstimate(
            flops=4 * tokens * rows * half,
            bytes_accessed=2 * tokens * hidden + 4 * rows * half,
            transcendentals=0,
        ),
    )(left, grads_out)


def keep_and_give(array, axis):
    half = array.shape[0] // 2
    low, high = array[:half], array[half:]
    first = lax.axis_index(axis) == 0
    return jnp.where(first, low, high), jnp.where(first, high, low)


def owned_sum(left, grads_out, axis, pair):
    count = lax.axis_size(axis)
    far = count // 2
    swaps = [
        [(i, (i + step) % count) for i in range(count) for step in (1 if (i + k) % 2 == 0 else -1,)]
        for k in range(2)
    ]
    across = [(0, 1), (1, 0)]
    line = left.shape[0] // (2 * count)
    long, short = block_sums(left, grads_out, (far * line,) * 2)
    long, short = (a.reshape(-1, line, a.shape[1]) for a in (long, short))
    one, two = lax.ppermute(long[0], axis, swaps[0]), short[0]
    for s in range(1, far):
        one = one + long[s]
        if s == 1:
            one, two = lax.optimization_barrier((one, two))
        if s < far - 1:
            one = lax.ppermute(one, axis, swaps[s % 2])
        two = lax.ppermute(two, axis, swaps[(s + 1) % 2]) + short[s]
    kept, given = keep_and_give(one, pair)
    last = swaps[(far - 1) % 2]
    slant = [(p * count + i, q * count + j) for p, q in across for i, j in last]
    aside = lax.ppermute(given, (pair, axis), slant)
    along = lax.ppermute(kept, axis, last)
    kept, given = keep_and_give(two, pair)
    return along + aside + (kept + lax.ppermute(given, pair, across))


def mean_over(arrays, axis):
    count = lax.axis_size(axis)
    flat = jnp.concatenate([a.reshape(-1) for a in arrays])
    tiles = flat.reshape(count, -1)
    arrived = lax.all_to_all(tiles, axis, 0, 0, tiled=True).sum(axis=0) / count
    whole = lax.all_to_all(
        jnp.broadcast_to(arrived[None], tiles.shape), axis, 0, 0, tiled=True
    ).reshape(-1)
    size = arrays[0].size
    return [whole[i * size : (i + 1) * size].reshape(a.shape) for i, a in enumerate(arrays)]


def per_device(activations, out_grads, params, first_moment, second_moment):
    blocks = lax.axis_size("z")
    feats, grads_out = activations[0], out_grads[0]
    shape = params.shape[1:]
    here = lax.axis_index("z")
    side = 1 - 2 * lax.rem(here, 2)
    far = blocks // 2

    def place(i):
        late = i // far
        sign = 2 * (i & 1) - 1
        return (here + side * (far + sign * (i % far + late))) & (blocks - 1)

    left = spread(feats, blocks, place)
    grad = owned_sum(left, grads_out, "z", "x")

    def fold(a):
        return a[0].reshape(grad.shape)

    weights, moment_one, moment_two = fold(params), fold(first_moment), fold(second_moment)
    new_first = 0.9 * moment_one + 0.1 * grad
    new_second = 0.95 * moment_two + 0.05 * grad * grad
    corr_first = 1.0 - 0.9**STEP
    corr_second = 1.0 - 0.95**STEP
    update = new_first / corr_first / (jnp.sqrt(new_second / corr_second) + 1e-08)
    new_params = weights - 0.01 * (update + 0.1 * weights)
    means = mean_over((new_params, new_first, new_second), "rep")
    return tuple(a.reshape(shape) for a in means)


def solution(mesh):
    split = Mesh(mesh.devices.reshape(mesh.shape["rep"], 2, 16), ("rep", "x", "z"))
    spec = P("rep", FSDP, None)
    out = P(FSDP, None)
    return jax.shard_map(
        per_device,
        mesh=split,
        in_specs=(spec,) * 5,
        out_specs=(out,) * 3,
        check_vma=False,
    )
```

```python
import jax
import jax.numpy as jnp
from jax import lax
from jax.sharding import Mesh
from jax.sharding import PartitionSpec as P

STEP = 100
FSDP = ("x", "z")


def contract_tokens(left, right):
    return lax.dot_general(
        left, right, (((0,), (0,)), ((), ())), preferred_element_type=jnp.float32
    )


def spread(feats, blocks, place):
    tokens, width = feats.shape
    rows = width // (2 * blocks)
    shape = (width, 4 * width)
    source, column = (lax.broadcasted_iota(jnp.int32, shape, i) for i in range(2))
    group = column // (2 * width)
    block = (column // (4 * rows)) % blocks
    pair = (column // (2 * rows)) % 2
    row = (column // 2) % rows
    wanted = (pair * blocks + place(block)) * rows + row
    chosen = (source == wanted) & (group == column % 2)
    picked = jnp.dot(feats, chosen.astype(feats.dtype), preferred_element_type=jnp.float32)
    return picked.astype(feats.dtype).reshape(tokens, 2, blocks, -1)


def block_sums(left, grads_out):
    half = grads_out.shape[1] // 2
    total = sum(
        contract_tokens(
            left[:, h].reshape(left.shape[0], -1),
            lax.slice_in_dim(grads_out, h * half, (h + 1) * half, axis=1),
        )
        for h in range(2)
    )
    return total.reshape(left.shape[2], -1, half)


def keep_and_give(array, axis):
    half = array.shape[0] // 2
    low, high = array[:half], array[half:]
    first = lax.axis_index(axis) == 0
    return jnp.where(first, low, high), jnp.where(first, high, low)


def owned_sum(left, grads_out, axis, pair):
    count = lax.axis_size(axis)
    far = count // 2
    swaps = [
        [(i, (i + step) % count) for i in range(count) for step in (1 if (i + k) % 2 == 0 else -1,)]
        for k in range(2)
    ]
    across = [(0, 1), (1, 0)]
    start = block_sums(left[:, :, :1], grads_out)[0]
    start, left = lax.optimization_barrier((start, left))
    one = lax.ppermute(start, axis, swaps[0])
    two = block_sums(left[:, :, far : far + 1], grads_out)[0]
    long = block_sums(left[:, :, 1:far], grads_out)
    two, long = lax.optimization_barrier((two, long))
    one, left = lax.optimization_barrier((one, left))
    short = block_sums(left[:, :, far + 1 :], grads_out)
    for s in range(1, far):
        one = one + long[s - 1]
        if s < far - 1:
            one = lax.ppermute(one, axis, swaps[s % 2])
        two = lax.ppermute(two, axis, swaps[(s + 1) % 2]) + short[s - 1]
    kept, given = keep_and_give(one, pair)
    last = swaps[(far - 1) % 2]
    slant = [(p * count + i, q * count + j) for p, q in across for i, j in last]
    aside = lax.ppermute(given, (pair, axis), slant)
    along = lax.ppermute(kept, axis, last)
    kept, given = keep_and_give(two, pair)
    return along + aside + (kept + lax.ppermute(given, pair, across))


def mean_over(arrays, axis):
    count = lax.axis_size(axis)
    flat = jnp.concatenate([a.reshape(-1) for a in arrays])
    tiles = flat.reshape(count, -1)
    arrived = lax.all_to_all(tiles, axis, 0, 0, tiled=True).sum(axis=0) / count
    whole = lax.all_to_all(
        jnp.broadcast_to(arrived[None], tiles.shape), axis, 0, 0, tiled=True
    ).reshape(-1)
    size = arrays[0].size
    return [whole[i * size : (i + 1) * size].reshape(a.shape) for i, a in enumerate(arrays)]


def per_device(activations, out_grads, params, first_moment, second_moment):
    blocks = lax.axis_size("z")
    feats, grads_out = activations[0], out_grads[0]
    shape = params.shape[1:]
    here = lax.axis_index("z")
    side = 1 - 2 * lax.rem(here, 2)
    far = blocks // 2

    def place(i):
        late = i // far
        sign = 2 * (i & 1) - 1
        return (here + side * (far + sign * (i % far + late))) & (blocks - 1)

    left = spread(feats, blocks, place)
    grad = owned_sum(left, grads_out, "z", "x")

    def fold(a):
        return a[0].reshape(grad.shape)

    weights, moment_one, moment_two = fold(params), fold(first_moment), fold(second_moment)
    new_first = 0.9 * moment_one + 0.1 * grad
    new_second = 0.95 * moment_two + 0.05 * grad * grad
    corr_first = 1.0 - 0.9**STEP
    corr_second = 1.0 - 0.95**STEP
    update = new_first / corr_first / (jnp.sqrt(new_second / corr_second) + 1e-08)
    new_params = weights - 0.01 * (update + 0.1 * weights)
    means = mean_over((new_params, new_first, new_second), "rep")
    return tuple(a.reshape(shape) for a in means)


def solution(mesh):
    split = Mesh(mesh.devices.reshape(mesh.shape["rep"], 2, 16), ("rep", "x", "z"))
    spec = P("rep", FSDP, None)
    out = P(FSDP, None)
    return jax.shard_map(
        per_device,
        mesh=split,
        in_specs=(spec,) * 5,
        out_specs=(out,) * 3,
        check_vma=False,
    )
```

```python
import jax
import jax.numpy as jnp
from jax import lax
from jax.sharding import Mesh
from jax.sharding import PartitionSpec as P

STEP = 100
FSDP = ("x", "z")


def contract_tokens(left, right):
    return lax.dot_general(
        left, right, (((0,), (0,)), ((), ())), preferred_element_type=jnp.float32
    )


def spread(feats, blocks, place):
    tokens, width = feats.shape
    rows = width // (2 * blocks)
    shape = (width, 4 * width)
    source, column = (lax.broadcasted_iota(jnp.int32, shape, i) for i in range(2))
    group = column // (2 * width)
    block = (column // (4 * rows)) % blocks
    pair = (column // (2 * rows)) % 2
    row = (column // 2) % rows
    wanted = (pair * blocks + place(block)) * rows + row
    chosen = (source == wanted) & (group == column % 2)
    picked = jnp.dot(feats, chosen.astype(feats.dtype), preferred_element_type=jnp.float32)
    return picked.astype(feats.dtype).reshape(tokens, 2, blocks, -1)


def block_sums(left, grads_out):
    half = grads_out.shape[1] // 2
    total = sum(
        contract_tokens(
            left[:, h].reshape(left.shape[0], -1),
            lax.slice_in_dim(grads_out, h * half, (h + 1) * half, axis=1),
        )
        for h in range(2)
    )
    return total.reshape(left.shape[2], -1, half)


def keep_and_give(array, axis):
    half = array.shape[0] // 2
    low, high = array[:half], array[half:]
    first = lax.axis_index(axis) == 0
    return jnp.where(first, low, high), jnp.where(first, high, low)


def owned_sum(left, grads_out, axis, pair):
    count = lax.axis_size(axis)
    far = count // 2
    swaps = [
        [(i, (i + step) % count) for i in range(count) for step in (1 if (i + k) % 2 == 0 else -1,)]
        for k in range(2)
    ]
    across = [(0, 1), (1, 0)]
    start = block_sums(left[:, :, :1], grads_out)[0]
    start, left = lax.optimization_barrier((start, left))
    one = lax.ppermute(start, axis, swaps[0])
    short = block_sums(left[:, :, far : far + 2], grads_out)
    long = block_sums(left[:, :, 1:far], grads_out)
    two, long = lax.optimization_barrier((short[0], long))
    short = [*short]
    for s in range(1, far):
        one = one + long[s - 1]
        if s < far - 1:
            one = lax.ppermute(one, axis, swaps[s % 2])
        two = lax.ppermute(two, axis, swaps[(s + 1) % 2])
        if s == 2:
            two, left = lax.optimization_barrier((two, left))
            short += [*block_sums(left[:, :, far + 2 :], grads_out)]
        two = two + short[s]
    kept, given = keep_and_give(one, pair)
    last = swaps[(far - 1) % 2]
    slant = [(p * count + i, q * count + j) for p, q in across for i, j in last]
    aside = lax.ppermute(given, (pair, axis), slant)
    along = lax.ppermute(kept, axis, last)
    kept, given = keep_and_give(two, pair)
    return along + aside + (kept + lax.ppermute(given, pair, across))


def mean_over(arrays, axis):
    count = lax.axis_size(axis)
    flat = jnp.concatenate([a.reshape(-1) for a in arrays])
    tiles = flat.reshape(count, -1)
    arrived = lax.all_to_all(tiles, axis, 0, 0, tiled=True).sum(axis=0) / count
    whole = lax.all_to_all(
        jnp.broadcast_to(arrived[None], tiles.shape), axis, 0, 0, tiled=True
    ).reshape(-1)
    size = arrays[0].size
    return [whole[i * size : (i + 1) * size].reshape(a.shape) for i, a in enumerate(arrays)]


def per_device(activations, out_grads, params, first_moment, second_moment):
    blocks = lax.axis_size("z")
    feats, grads_out = activations[0], out_grads[0]
    shape = params.shape[1:]
    here = lax.axis_index("z")
    side = 1 - 2 * lax.rem(here, 2)
    far = blocks // 2

    def place(i):
        late = i // far
        sign = 2 * (i & 1) - 1
        return (here + side * (far + sign * (i % far + late))) & (blocks - 1)

    left = spread(feats, blocks, place)
    grad = owned_sum(left, grads_out, "z", "x")

    def fold(a):
        return a[0].reshape(grad.shape)

    weights, moment_one, moment_two = fold(params), fold(first_moment), fold(second_moment)
    new_first = 0.9 * moment_one + 0.1 * grad
    new_second = 0.95 * moment_two + 0.05 * grad * grad
    corr_first = 1.0 - 0.9**STEP
    corr_second = 1.0 - 0.95**STEP
    update = new_first / corr_first / (jnp.sqrt(new_second / corr_second) + 1e-08)
    new_params = weights - 0.01 * (update + 0.1 * weights)
    means = mean_over((new_params, new_first, new_second), "rep")
    return tuple(a.reshape(shape) for a in means)


def solution(mesh):
    split = Mesh(mesh.devices.reshape(mesh.shape["rep"], 2, 16), ("rep", "x", "z"))
    spec = P("rep", FSDP, None)
    out = P(FSDP, None)
    return jax.shard_map(
        per_device,
        mesh=split,
        in_specs=(spec,) * 5,
        out_specs=(out,) * 3,
        check_vma=False,
    )
```
